32 devices in a mesh: row: 8 (over z, x), col: 4 (over y, core).
Axes of the slice: x: 2, y: 2, z: 4, core: 2. Of those that a mesh axis runs over, the one named last changes fastest.
Arguments:
- normal_matrix: float32 [4096, 4096], P('row', 'col'), as said below
Outputs:
- factored: float32 [4096, 4096], P('row', 'col')
- log_det: float32 [], replicated
Inputs may be any that keep to these rules, and one draw needn't show every extreme that they name: normal_matrix is symmetric and positive definite.
All inputs are finite; a program needn't handle non-finite values.
Results may differ from the reference program's by a relative error of at most 0.0001.
Values sent between devices are 32-bit elements; how exact they have to be, the bound alone decides.
No kernel may reach another device: no remote copies, remote signals or barrier semaphores. Data moves between devices by JAX's collectives and lax.ppermute only.
A program may use at most 64 MiB of HBM per device.

```python
import math
import jax
import jax.numpy as jnp
from jax import lax

B = 512
STEPS = 1
N = 4096


def draw_normal_matrix(key, part):
    key_green = jax.random.fold_in(key, 21)
    key_diag = jax.random.fold_in(key, 22)
    key_scale = jax.random.fold_in(key, 23)
    key_weight = jax.random.fold_in(key, 24)
    observe = 2 * B
    position = jnp.arange(N, dtype=jnp.float32) / N
    rising = jnp.exp(position * math.log(3.0))
    green = jax.random.normal(key_green, (observe, N), jnp.float32)
    data_weight = jnp.exp(jax.random.uniform(key_weight, (observe,), jnp.float32, math.log(0.7), math.log(1.4)))
    diag_add = jax.random.uniform(key_diag, (N,), jnp.float32, 0.5, 2.5)
    rough = jnp.exp(jax.random.uniform(key_scale, (N,), jnp.float32, 0.0, math.log(2.0)))
    scales = 0.6 * rising * rough
    weighted = green * (data_weight / math.sqrt(observe))[:, None]
    gram = jnp.dot(weighted.T, weighted, precision=lax.Precision.HIGHEST)
    base = 0.5 * (gram + gram.T) + jnp.diag(diag_add)
    return base * (scales[:, None] * scales[None, :])


def setup_inputs(seed: int = 0) -> dict:
    key_of = jax.random.split(jax.random.key(seed), 2)
    return {
        "normal_matrix": draw_normal_matrix(jax.random.fold_in(key_of[1], 71), 0),
    }


def reference(normal_matrix):
    matrix = normal_matrix
    log_det = jnp.float32(0.0)
    for panel_step in range(STEPS):
        start_at = panel_step * B
        end_at = start_at + B
        factor = jnp.linalg.cholesky(matrix[start_at:end_at, start_at:end_at])
        panel_cols = jax.scipy.linalg.solve_triangular(factor, matrix[end_at:, start_at:end_at].T, lower=True).T
        update = jnp.dot(panel_cols, panel_cols.T, precision=lax.Precision.HIGHEST)
        matrix = matrix.at[end_at:, end_at:].add(-update)
        matrix = matrix.at[end_at:, start_at:end_at].set(panel_cols)
        matrix = matrix.at[start_at:end_at, start_at:end_at].set(factor)
        matrix = matrix.at[start_at:end_at, end_at:].set(jnp.float32(0.0))
        log_det = log_det + 2.0 * jnp.sum(jnp.log(jnp.diagonal(factor)))
    return (matrix, log_det)
```

```python
import jax
import jax.numpy as jnp
from jax import lax
from jax.experimental import pallas as pl
from jax.experimental.pallas import tpu as pltpu
from jax.sharding import PartitionSpec as P

LANES = 128
SUB = 8
TILES = LANES // SUB
GROUP = 4


def block_index(k, j, count):
    return k * count - (k * (k - 1)) // 2 + (j - k)


def leaf(a_ref, w_ref, base):
    a = [a_ref[base + t] for t in range(TILES)]
    sub = lax.broadcasted_iota(jnp.int32, (SUB, LANES), 0)
    lane = lax.broadcasted_iota(jnp.int32, (SUB, LANES), 1)
    w = [jnp.where(lane == sub + SUB * t, 1.0, 0.0).astype(jnp.float32) for t in range(TILES)]
    logs = jnp.zeros((SUB, LANES), jnp.float32)
    shape = (SUB, LANES)
    for g in range(LANES // GROUP):
        i, q, first = (GROUP * g) // SUB, (GROUP * g) % SUB, GROUP * g
        rows = [jnp.broadcast_to(a[i][q + k : q + k + 1, :], shape) for k in range(GROUP)]
        wrows = [jnp.broadcast_to(w[i][q + k : q + k + 1, :], shape) for k in range(GROUP)]
        piv = {
            (k, l): jnp.broadcast_to(rows[k][:, first + l : first + l + 1], shape)
            for k in range(GROUP)
            for l in range(k, GROUP)
        }
        scale, inv, mult = [], [], {}
        for k in range(GROUP):
            s = lax.rsqrt(piv[k, k])
            logs = logs + jnp.log(piv[k, k])
            scale.append(s)
            inv.append(s * s)
            for l in range(k + 1, GROUP):
                mult[l, k] = piv[k, l] * inv[k]
            for l in range(k + 1, GROUP):
                for m in range(l, GROUP):
                    piv[l, m] = piv[l, m] - mult[l, k] * piv[k, m]
            for l in range(k + 1, GROUP):
                rows[l] = rows[l] - mult[l, k] * rows[k]
                wrows[l] = wrows[l] - mult[l, k] * wrows[k]
        for k in range(GROUP):
            w_ref[base + i, q + k : q + k + 1, :] = (wrows[k] * scale[k])[0:1, :]
        start = i if q + GROUP < SUB else i + 1
        if start >= TILES:
            continue
        ya = [rows[k] * inv[k] for k in range(GROUP)]
        yw = [wrows[k] * inv[k] for k in range(GROUP)]
        for k in range(GROUP - 1, 0, -1):
            for l in range(k):
                ya[l] = ya[l] - mult[k, l] * ya[k]
                yw[l] = yw[l] - mult[k, l] * yw[k]
        for t in range(start, TILES):
            cols = [jnp.broadcast_to(a[t][:, first + k : first + k + 1], shape) for k in range(GROUP)]
            da = (cols[0] * ya[0] + cols[1] * ya[1]) + (cols[2] * ya[2] + cols[3] * ya[3])
            dw = (cols[0] * yw[0] + cols[1] * yw[1]) + (cols[2] * yw[2] + cols[3] * yw[3])
            a[t] = a[t] - da
            w[t] = w[t] - dw
    return logs


def mm(x, y, dims):
    return lax.dot_general(
        x, y, (dims, ((), ())), precision=lax.Precision.HIGHEST, preferred_element_type=jnp.float32
    )


def panels_body(first, last, count, a_in, w_in, log_in, a, w, log):
    def get(ref, b):
        return ref[b * TILES : (b + 1) * TILES].reshape(LANES, LANES)

    def put(ref, b, value):
        ref[b * TILES : (b + 1) * TILES] = value.reshape(TILES, SUB, LANES)

    a[...] = a_in[...]
    w[...] = w_in[...]
    log[...] = log_in[...]

    def step(k, carry):
        base = TILES * (k * count - (k * (k - 1)) // 2)
        log[...] = log[...] + leaf(a, w, base)
        for kk in range(first, last):

            @pl.when(k == kk)
            def _():
                inv = get(w, block_index(kk, kk, count))
                right = list(range(kk + 1, count))
                left = list(range(kk))
                src = [get(a, block_index(kk, j, count)) for j in right]
                src += [get(w, block_index(j, kk, count)) for j in left]
                if not src:
                    return
                out = mm(inv, jnp.concatenate(src, axis=1), ((1,), (0,)))
                parts = [out[:, n * LANES : (n + 1) * LANES] for n in range(len(src))]
                upper = dict(zip(right, parts[: len(right)]))
                lower = dict(zip(left, parts[len(right) :]))
                for j in left:
                    put(w, block_index(j, kk, count), lower[j])
                lower[kk] = inv
                for i in right:
                    cols = [upper[j] for j in right if j >= i] + [lower[j] for j in range(kk + 1)]
                    upd = mm(upper[i], jnp.concatenate(cols, axis=1), ((0,), (0,)))
                    n = 0
                    for j in right:
                        if j >= i:
                            b = block_index(i, j, count)
                            put(a, b, get(a, b) - upd[:, n * LANES : (n + 1) * LANES])
                            n += 1
                    for j in range(kk + 1):
                        b = block_index(j, i, count)
                        old = get(w, b) if j < kk else jnp.zeros((LANES, LANES), jnp.float32)
                        put(w, b, old - upd[:, n * LANES : (n + 1) * LANES])
                        n += 1

        return carry

    lax.fori_loop(first, last, step, 0)


def panels(first, last, count, a, w, log):
    def body(a_in, w_in, log_in, a_out, w_out, log_out):
        panels_body(first, last, count, a_in, w_in, log_in, a_out, w_out, log_out)

    shapes = [jax.ShapeDtypeStruct(x.shape, jnp.float32) for x in (a, w, log)]
    return pl.pallas_call(body, out_shape=shapes, name=f"panels_{first}")(a, w, log)


def spread_from_first(value, axis):
    size = lax.axis_size(axis)
    index = lax.axis_index(axis)
    stride = 1
    while stride < size:
        stride *= 2
    stride //= 2
    while stride >= 1:
        step = 2 * stride
        pairs = [(s, s + stride) for s in range(0, size, step) if s + stride < size]
        got = lax.ppermute(value, axis, pairs)
        value = jnp.where(index % step == stride, got, value)
        stride //= 2
    return value


def per_device(block):
    width, cols = block.shape
    both = ("row", "col")
    rows_n = lax.axis_size("row")
    devices = rows_n * lax.axis_size("col")
    row = lax.axis_index("row")
    col = lax.axis_index("col")
    count = width // LANES

    packed = jnp.stack(
        [
            block[k * LANES : (k + 1) * LANES, j * LANES : (j + 1) * LANES]
            for k in range(count)
            for j in range(k, count)
        ]
    ).reshape(-1, SUB, LANES)
    tiles = packed.shape[0]
    per = -(-tiles // devices)
    sent = jnp.pad(packed, ((0, per * devices - tiles), (0, 0), (0, 0)))
    sent = sent.reshape(devices, per, SUB, LANES)
    mine = lax.all_to_all(sent, both, 0, 0)[0]
    diag = lax.all_gather(mine, both, axis=0, tiled=True)[:tiles]

    tied, diag = lax.optimization_barrier((block, diag))
    own = spread_from_first(tied[:, :width], "col")
    piece_rows = width // rows_n
    piece = tied[:piece_rows]
    for t in range(1, rows_n):
        got = lax.ppermute(tied[t * piece_rows : (t + 1) * piece_rows], "row", [(0, t)])
        piece = jnp.where(row == t, got, piece)

    log = jnp.zeros((SUB, LANES), jnp.float32)
    half = (count + 1) // 2
    a, w, log = panels(0, half, count, diag, jnp.zeros_like(diag), log)
    piece, own, a = lax.optimization_barrier((piece, own, a))

    top = jnp.zeros((rows_n, piece_rows, cols), jnp.float32)
    top = lax.dynamic_update_slice(top, piece[None], (row, 0, 0))
    for s in range(1, rows_n):
        got = lax.ppermute(piece, "row", [(i, (i + s) % rows_n) for i in range(rows_n)])
        top = lax.dynamic_update_slice(top, got[None], ((row - s) % rows_n, 0, 0))
    top = top.reshape(width, cols)

    a, w, log = panels(half, count, count, a, w, log)
    w_blocks = w.reshape(-1, LANES, LANES)
    zero = jnp.zeros((LANES, LANES), jnp.float32)
    inverse = jnp.concatenate(
        [
            jnp.concatenate(
                [w_blocks[block_index(j, i, count)] if j <= i else zero for j in range(count)], axis=1
            )
            for i in range(count)
        ],
        axis=0,
    )
    high = lax.Precision.HIGH
    panel = lax.dot_general(own, inverse, (((1,), (1,)), ((), ())), precision=high)
    upper = jnp.dot(inverse, top, precision=high)
    update = jnp.dot(panel, upper, precision=high)
    col_block = (cols // width) * col + jnp.arange(cols, dtype=jnp.int32) // width
    first_col = (col_block == 0)[None, :]
    in_row = jnp.arange(width, dtype=jnp.int32)
    keep = (row > 0) | (in_row[:, None] >= in_row[None, :])
    panel = jnp.where(keep, panel, 0.0)
    panel = jnp.concatenate([panel] * (cols // width), axis=1)
    rest = jnp.where(row > 0, block - update, 0.0)
    return jnp.where(first_col, panel, rest), log[0, 0]


def solution(mesh):
    return jax.shard_map(
        per_device,
        mesh=mesh,
        in_specs=(P("row", "col"),),
        out_specs=(P("row", "col"), P()),
        check_vma=False,
    )
```

```python
import jax
import jax.numpy as jnp
from jax import lax
from jax.experimental import pallas as pl
from jax.experimental.pallas import tpu as pltpu
from jax.sharding import PartitionSpec as P

LANES = 128
SUB = 8
TILES = LANES // SUB
GROUP = 4


def block_index(k, j, count):
    return k * count - (k * (k - 1)) // 2 + (j - k)


def leaf(a_ref, w_ref, base):
    a = [a_ref[base + t] for t in range(TILES)]
    sub = lax.broadcasted_iota(jnp.int32, (SUB, LANES), 0)
    lane = lax.broadcasted_iota(jnp.int32, (SUB, LANES), 1)
    w = [jnp.where(lane == sub + SUB * t, 1.0, 0.0).astype(jnp.float32) for t in range(TILES)]
    logs = jnp.zeros((SUB, LANES), jnp.float32)
    shape = (SUB, LANES)
    for g in range(LANES // GROUP):
        i, q, first = (GROUP * g) // SUB, (GROUP * g) % SUB, GROUP * g
        rows = [jnp.broadcast_to(a[i][q + k : q + k + 1, :], shape) for k in range(GROUP)]
        wrows = [jnp.broadcast_to(w[i][q + k : q + k + 1, :], shape) for k in range(GROUP)]
        piv = {
            (k, l): jnp.broadcast_to(rows[k][:, first + l : first + l + 1], shape)
            for k in range(GROUP)
            for l in range(k, GROUP)
        }
        scale, inv, mult = [], [], {}
        for k in range(GROUP):
            s = lax.rsqrt(piv[k, k])
            logs = logs + jnp.log(piv[k, k])
            scale.append(s)
            inv.append(s * s)
            for l in range(k + 1, GROUP):
                mult[l, k] = piv[k, l] * inv[k]
            for l in range(k + 1, GROUP):
                for m in range(l, GROUP):
                    piv[l, m] = piv[l, m] - mult[l, k] * piv[k, m]
            for l in range(k + 1, GROUP):
                rows[l] = rows[l] - mult[l, k] * rows[k]
                wrows[l] = wrows[l] - mult[l, k] * wrows[k]
        for k in range(GROUP):
            w_ref[base + i, q + k : q + k + 1, :] = (wrows[k] * scale[k])[0:1, :]
        start = i if q + GROUP < SUB else i + 1
        if start >= TILES:
            continue
        ya = [rows[k] * inv[k] for k in range(GROUP)]
        yw = [wrows[k] * inv[k] for k in range(GROUP)]
        for k in range(GROUP - 1, 0, -1):
            for l in range(k):
                ya[l] = ya[l] - mult[k, l] * ya[k]
                yw[l] = yw[l] - mult[k, l] * yw[k]
        for t in range(start, TILES):
            cols = [jnp.broadcast_to(a[t][:, first + k : first + k + 1], shape) for k in range(GROUP)]
            da = (cols[0] * ya[0] + cols[1] * ya[1]) + (cols[2] * ya[2] + cols[3] * ya[3])
            dw = (cols[0] * yw[0] + cols[1] * yw[1]) + (cols[2] * yw[2] + cols[3] * yw[3])
            a[t] = a[t] - da
            w[t] = w[t] - dw
    return logs


def mm(x, y, dims):
    return lax.dot_general(
        x, y, (dims, ((), ())), precision=lax.Precision.HIGHEST, preferred_element_type=jnp.float32
    )


def get(ref, b):
    return ref[b * TILES : (b + 1) * TILES].reshape(LANES, LANES)


def put(ref, b, value):
    ref[b * TILES : (b + 1) * TILES] = value.reshape(TILES, SUB, LANES)


def row_panel(kk, count, a, w):
    inv = get(w, block_index(kk, kk, count))
    right, left = list(range(kk + 1, count)), list(range(kk))
    src = [get(a, block_index(kk, j, count)) for j in right]
    src += [get(w, block_index(j, kk, count)) for j in left]
    if not src:
        return
    out = mm(inv, jnp.concatenate(src, axis=1), ((1,), (0,)))
    for n, j in enumerate(right):
        put(a, block_index(kk, j, count), out[:, n * LANES : (n + 1) * LANES])
    for n, j in enumerate(left, len(right)):
        put(w, block_index(j, kk, count), out[:, n * LANES : (n + 1) * LANES])


def trail(kk, count, a, w):
    for i in range(kk + 1, count):
        cols = [get(a, block_index(kk, j, count)) for j in range(i, count)]
        cols += [get(w, block_index(j, kk, count)) for j in range(kk + 1)]
        upd = mm(get(a, block_index(kk, i, count)), jnp.concatenate(cols, axis=1), ((0,), (0,)))
        n = 0
        for j in range(i, count):
            b = block_index(i, j, count)
            put(a, b, get(a, b) - upd[:, n * LANES : (n + 1) * LANES])
            n += 1
        for j in range(kk + 1):
            b = block_index(j, i, count)
            old = get(w, b) if j < kk else jnp.zeros((LANES, LANES), jnp.float32)
            put(w, b, old - upd[:, n * LANES : (n + 1) * LANES])
            n += 1


def first_panel(top, count):
    def body(top_ref, out, inv, log, a, w):
        for j in range(count):
            put(a, j, top_ref[:, j * LANES : (j + 1) * LANES])
        log[...] = leaf(a, w, 0)
        row_panel(0, count, a, w)
        for j in range(1, count):
            out[:, j * LANES : (j + 1) * LANES] = get(a, j)
        out[:, :LANES] = jnp.zeros((LANES, LANES), jnp.float32)
        inv[...] = get(w, 0)

    f32 = jnp.float32
    return pl.pallas_call(
        body,
        out_shape=[
            jax.ShapeDtypeStruct((LANES, count * LANES), f32),
            jax.ShapeDtypeStruct((LANES, LANES), f32),
            jax.ShapeDtypeStruct((SUB, LANES), f32),
        ],
        scratch_shapes=[
            pltpu.VMEM((count * TILES, SUB, LANES), f32),
            pltpu.VMEM((TILES, SUB, LANES), f32),
        ],
        name="first_panel",
    )(top)


def other_panels(top, inv, log, rest, count):
    blocks = count * (count + 1) // 2

    def body(top_ref, inv_ref, log_ref, rest_ref, inverse, log, a, w):
        for j in range(1, count):
            put(a, j, top_ref[:, j * LANES : (j + 1) * LANES])
        for b in range(count, blocks):
            n = b - count
            put(a, b, rest_ref[:, n * LANES : (n + 1) * LANES])
        put(w, 0, inv_ref[...])
        log[...] = log_ref[...]
        trail(0, count, a, w)

        def step(k, carry):
            base = TILES * (k * count - (k * (k - 1)) // 2)
            log[...] = log[...] + leaf(a, w, base)
            for kk in range(1, count):

                @pl.when(k == kk)
                def _():
                    row_panel(kk, count, a, w)
                    trail(kk, count, a, w)

            return carry

        lax.fori_loop(1, count, step, 0)
        for i in range(count):
            for j in range(count):
                value = get(w, block_index(j, i, count)) if j <= i else jnp.zeros((LANES, LANES), jnp.float32)
                inverse[i * LANES : (i + 1) * LANES, j * LANES : (j + 1) * LANES] = value

    f32 = jnp.float32
    return pl.pallas_call(
        body,
        out_shape=[
            jax.ShapeDtypeStruct((count * LANES, count * LANES), f32),
            jax.ShapeDtypeStruct((SUB, LANES), f32),
        ],
        scratch_shapes=[
            pltpu.VMEM((blocks * TILES, SUB, LANES), f32),
            pltpu.VMEM((blocks * TILES, SUB, LANES), f32),
        ],
        name="other_panels",
    )(top, inv, log, rest)


def tree_rounds(value, axes, strides):
    index = lax.axis_index(axes)
    size = lax.axis_size(axes)
    have = [0]
    for stride in strides:
        got = lax.ppermute(value, axes, [(s, s + stride) for s in have])
        value = jnp.where((index // stride) % 2 == 1, got, value)
        have = have + [s + stride for s in have]
    assert len(have) == size
    return value


def halvings(size, unit=1):
    out = []
    while size > 1:
        size //= 2
        out.append(size * unit)
    return out


def per_device(block):
    width, cols = block.shape
    both = ("row", "col")
    rows_n, cols_n = lax.axis_size("row"), lax.axis_size("col")
    row = lax.axis_index("row")
    col = lax.axis_index("col")
    count = width // LANES
    per_col = cols // width

    first = block[:LANES, :width]
    rest = jnp.concatenate(
        [block[k * LANES : (k + 1) * LANES, k * LANES : width] for k in range(1, count)], axis=1
    )
    row_strides, col_strides = halvings(rows_n, cols_n), halvings(cols_n)
    first = tree_rounds(first, both, row_strides + col_strides)
    rest = tree_rounds(rest, both, col_strides[:-1] + row_strides[::-1] + col_strides[-1:])

    held = block[:, :width]
    piece_rows = width // rows_n
    pieces = held.reshape(rows_n, piece_rows, width)
    slots = [jnp.zeros((piece_rows, width), jnp.float32) for _ in range(per_col)]
    for s in range(rows_n):
        mine = lax.dynamic_index_in_dim(pieces, (row + s) % rows_n, 0, keepdims=False)
        pairs = [
            (r * cols_n, ((r + s) % rows_n) * cols_n + r // per_col) for r in range(rows_n)
        ]
        got = lax.ppermute(mine, both, pairs)
        slots = [
            jnp.where((row - per_col * col - b) % rows_n == s, got, slots[b]) for b in range(per_col)
        ]
    piece = jnp.stack(slots)[:, None]
    own = tree_rounds(held, "col", col_strides)

    far = jnp.zeros((per_col, rows_n, piece_rows, width), jnp.float32)
    far = lax.dynamic_update_slice(far, piece, (0, row, 0, 0))
    for s in range(1, rows_n):
        got = lax.ppermute(piece, "row", [(i, (i + s) % rows_n) for i in range(rows_n)])
        far = lax.dynamic_update_slice(far, got, (0, (row - s) % rows_n, 0, 0))
    far = far.reshape(cols, width)

    top, inv, log = first_panel(first, count)
    inverse, log = other_panels(top, inv, log, rest, count)

    high = lax.Precision.HIGH
    across = (((1,), (1,)), ((), ()))
    panel = lax.dot_general(own, inverse, across, precision=high)
    other = lax.dot_general(far, inverse, across, precision=high)
    update = lax.dot_general(panel, other, across, precision=high)
    col_block = per_col * col + jnp.arange(cols, dtype=jnp.int32) // width
    first_col = (col_block == 0)[None, :]
    in_row = jnp.arange(width, dtype=jnp.int32)
    keep = (row > 0) | (in_row[:, None] >= in_row[None, :])
    panel = jnp.where(keep, panel, 0.0)
    panel = jnp.concatenate([panel] * per_col, axis=1)
    rest_out = jnp.where(row > 0, block - update, 0.0)
    return jnp.where(first_col, panel, rest_out), log[0, 0]


def solution(mesh):
    return jax.shard_map(
        per_device,
        mesh=mesh,
        in_specs=(P("row", "col"),),
        out_specs=(P("row", "col"), P()),
        check_vma=False,
    )
```

```python
import jax
import jax.numpy as jnp
from jax import lax
from jax.experimental import pallas as pl
from jax.experimental.pallas import tpu as pltpu
from jax.sharding import PartitionSpec as P

LANES = 128
SUB = 8
TILES = LANES // SUB
GROUP = 4


def block_index(k, j, count):
    return k * count - (k * (k - 1)) // 2 + (j - k)


def leaf(a_ref, w_ref, base):
    a = [a_ref[base + t] for t in range(TILES)]
    sub = lax.broadcasted_iota(jnp.int32, (SUB, LANES), 0)
    lane = lax.broadcasted_iota(jnp.int32, (SUB, LANES), 1)
    w = [jnp.where(lane == sub + SUB * t, 1.0, 0.0).astype(jnp.float32) for t in range(TILES)]
    logs = jnp.zeros((SUB, LANES), jnp.float32)
    shape = (SUB, LANES)
    for g in range(LANES // GROUP):
        i, q, first = (GROUP * g) // SUB, (GROUP * g) % SUB, GROUP * g
        rows = [jnp.broadcast_to(a[i][q + k : q + k + 1, :], shape) for k in range(GROUP)]
        wrows = [jnp.broadcast_to(w[i][q + k : q + k + 1, :], shape) for k in range(GROUP)]
        piv = {
            (k, l): jnp.broadcast_to(rows[k][:, first + l : first + l + 1], shape)
            for k in range(GROUP)
            for l in range(k, GROUP)
        }
        scale, inv, mult = [], [], {}
        for k in range(GROUP):
            s = lax.rsqrt(piv[k, k])
            logs = logs + jnp.log(piv[k, k])
            scale.append(s)
            inv.append(s * s)
            for l in range(k + 1, GROUP):
                mult[l, k] = piv[k, l] * inv[k]
            for l in range(k + 1, GROUP):
                for m in range(l, GROUP):
                    piv[l, m] = piv[l, m] - mult[l, k] * piv[k, m]
            for l in range(k + 1, GROUP):
                rows[l] = rows[l] - mult[l, k] * rows[k]
                wrows[l] = wrows[l] - mult[l, k] * wrows[k]
        for k in range(GROUP):
            w_ref[base + i, q + k : q + k + 1, :] = (wrows[k] * scale[k])[0:1, :]
        start = i if q + GROUP < SUB else i + 1
        if start >= TILES:
            continue
        ya = [rows[k] * inv[k] for k in range(GROUP)]
        yw = [wrows[k] * inv[k] for k in range(GROUP)]
        for k in range(GROUP - 1, 0, -1):
            for l in range(k):
                ya[l] = ya[l] - mult[k, l] * ya[k]
                yw[l] = yw[l] - mult[k, l] * yw[k]
        for t in range(start, TILES):
            cols = [jnp.broadcast_to(a[t][:, first + k : first + k + 1], shape) for k in range(GROUP)]
            da = (cols[0] * ya[0] + cols[1] * ya[1]) + (cols[2] * ya[2] + cols[3] * ya[3])
            dw = (cols[0] * yw[0] + cols[1] * yw[1]) + (cols[2] * yw[2] + cols[3] * yw[3])
            a[t] = a[t] - da
            w[t] = w[t] - dw
    return logs


def mm(x, y, dims):
    return lax.dot_general(
        x, y, (dims, ((), ())), precision=lax.Precision.HIGHEST, preferred_element_type=jnp.float32
    )


def get(ref, b):
    return ref[b * TILES : (b + 1) * TILES].reshape(LANES, LANES)


def put(ref, b, value):
    ref[b * TILES : (b + 1) * TILES] = value.reshape(TILES, SUB, LANES)


def row_panel(kk, count, a, w):
    inv = get(w, block_index(kk, kk, count))
    right, left = list(range(kk + 1, count)), list(range(kk))
    src = [get(a, block_index(kk, j, count)) for j in right]
    src += [get(w, block_index(j, kk, count)) for j in left]
    if not src:
        return
    out = mm(inv, jnp.concatenate(src, axis=1), ((1,), (0,)))
    for n, j in enumerate(right):
        put(a, block_index(kk, j, count), out[:, n * LANES : (n + 1) * LANES])
    for n, j in enumerate(left, len(right)):
        put(w, block_index(j, kk, count), out[:, n * LANES : (n + 1) * LANES])


def trail(kk, count, a, w):
    for i in range(kk + 1, count):
        cols = [get(a, block_index(kk, j, count)) for j in range(i, count)]
        cols += [get(w, block_index(j, kk, count)) for j in range(kk + 1)]
        upd = mm(get(a, block_index(kk, i, count)), jnp.concatenate(cols, axis=1), ((0,), (0,)))
        n = 0
        for j in range(i, count):
            b = block_index(i, j, count)
            put(a, b, get(a, b) - upd[:, n * LANES : (n + 1) * LANES])
            n += 1
        for j in range(kk + 1):
            b = block_index(j, i, count)
            old = get(w, b) if j < kk else jnp.zeros((LANES, LANES), jnp.float32)
            put(w, b, old - upd[:, n * LANES : (n + 1) * LANES])
            n += 1


def first_panel(top, count):
    def body(top_ref, out, inv, log, a, w):
        for j in range(count):
            put(a, j, top_ref[:, j * LANES : (j + 1) * LANES])
        log[...] = leaf(a, w, 0)
        row_panel(0, count, a, w)
        for j in range(1, count):
            out[:, j * LANES : (j + 1) * LANES] = get(a, j)
        out[:, :LANES] = jnp.zeros((LANES, LANES), jnp.float32)
        inv[...] = get(w, 0)

    f32 = jnp.float32
    return pl.pallas_call(
        body,
        out_shape=[
            jax.ShapeDtypeStruct((LANES, count * LANES), f32),
            jax.ShapeDtypeStruct((LANES, LANES), f32),
            jax.ShapeDtypeStruct((SUB, LANES), f32),
        ],
        scratch_shapes=[
            pltpu.VMEM((count * TILES, SUB, LANES), f32),
            pltpu.VMEM((TILES, SUB, LANES), f32),
        ],
        name="first_panel",
    )(top)


def other_panels(top, inv, log, rest, count):
    blocks = count * (count + 1) // 2

    def body(top_ref, inv_ref, log_ref, rest_ref, inverse, log, a, w):
        for j in range(1, count):
            put(a, j, top_ref[:, j * LANES : (j + 1) * LANES])
        for b in range(count, blocks):
            n = b - count
            put(a, b, rest_ref[:, n * LANES : (n + 1) * LANES])
        put(w, 0, inv_ref[...])
        log[...] = log_ref[...]
        trail(0, count, a, w)

        def step(k, carry):
            base = TILES * (k * count - (k * (k - 1)) // 2)
            log[...] = log[...] + leaf(a, w, base)
            for kk in range(1, count):

                @pl.when(k == kk)
                def _():
                    row_panel(kk, count, a, w)
                    trail(kk, count, a, w)

            return carry

        lax.fori_loop(1, count, step, 0)
        for i in range(count):
            for j in range(count):
                value = get(w, block_index(j, i, count)) if j <= i else jnp.zeros((LANES, LANES), jnp.float32)
                inverse[i * LANES : (i + 1) * LANES, j * LANES : (j + 1) * LANES] = value

    f32 = jnp.float32
    return pl.pallas_call(
        body,
        out_shape=[
            jax.ShapeDtypeStruct((count * LANES, count * LANES), f32),
            jax.ShapeDtypeStruct((SUB, LANES), f32),
        ],
        scratch_shapes=[
            pltpu.VMEM((blocks * TILES, SUB, LANES), f32),
            pltpu.VMEM((blocks * TILES, SUB, LANES), f32),
        ],
        name="other_panels",
    )(top, inv, log, rest)


def tree_rounds(value, axes, strides, have=(0,)):
    index = lax.axis_index(axes)
    have = list(have)
    for stride in strides:
        got = lax.ppermute(value, axes, [(s, s + stride) for s in have])
        value = jnp.where((index // stride) % 2 == 1, got, value)
        have = have + [s + stride for s in have]
    return value


def halvings(size, unit=1):
    out = []
    while size > 1:
        size //= 2
        out.append(size * unit)
    return out


def per_device(block):
    width, cols = block.shape
    both = ("row", "col")
    rows_n, cols_n = lax.axis_size("row"), lax.axis_size("col")
    row = lax.axis_index("row")
    col = lax.axis_index("col")
    count = width // LANES
    per_col = cols // width

    first = block[:LANES, :width]
    rest = jnp.concatenate(
        [block[k * LANES : (k + 1) * LANES, k * LANES : width] for k in range(1, count)], axis=1
    )
    row_strides, col_strides = halvings(rows_n, cols_n), halvings(cols_n)
    first = tree_rounds(first, both, row_strides)
    rest = tree_rounds(rest, both, col_strides[:-1] + row_strides[::-1] + col_strides[-1:])
    own = tree_rounds(block[:, :width], "col", col_strides[:-1])
    first, own = lax.optimization_barrier((first, own))
    own = tree_rounds(own, "col", col_strides[-1:], range(0, cols_n, 2))
    first = tree_rounds(first, both, col_strides, range(0, rows_n * cols_n, cols_n))

    far = own
    low, size = 0, 1
    while size < cols_n:
        moves = [
            (low + i, low - 1 - i if i < size // 2 else low + 2 * size - 1 - i) for i in range(size)
        ]
        if 2 * size == cols_n:
            first, far = lax.optimization_barrier((first, far))
        got = lax.ppermute(
            far,
            both,
            [
                (
                    (((c + src) % cols_n) * per_col + b) * cols_n + c,
                    (((c + dst) % cols_n) * per_col + b) * cols_n + c,
                )
                for c in range(cols_n)
                for b in range(per_col)
                for src, dst in moves
            ],
        )
        offset = (row // per_col - col) % cols_n
        takes = jnp.zeros((), bool)
        for _, dst in moves:
            takes = takes | (offset == dst % cols_n)
        far = jnp.where(takes, got, far)
        low, size = low - size // 2, 2 * size

    top, inv, log = first_panel(first, count)
    top, far = lax.optimization_barrier((top, far))
    parts = jnp.zeros((per_col, width, width), jnp.float32)
    parts = lax.dynamic_update_slice(parts, far[None], (row % per_col, 0, 0))
    for s in range(1, per_col):
        pairs = [(r, r - r % per_col + (r % per_col + s) % per_col) for r in range(rows_n)]
        got = lax.ppermute(far, "row", pairs)
        parts = lax.dynamic_update_slice(parts, got[None], ((row - s) % per_col, 0, 0))
    far = parts.reshape(cols, width)
    inverse, log = other_panels(top, inv, log, rest, count)

    high = lax.Precision.HIGH
    across = (((1,), (1,)), ((), ()))
    panel = lax.dot_general(own, inverse, across, precision=high)
    other = lax.dot_general(far, inverse, across, precision=high)
    update = lax.dot_general(panel, other, across, precision=high)
    col_block = per_col * col + jnp.arange(cols, dtype=jnp.int32) // width
    first_col = (col_block == 0)[None, :]
    in_row = jnp.arange(width, dtype=jnp.int32)
    keep = (row > 0) | (in_row[:, None] >= in_row[None, :])
    panel = jnp.where(keep, panel, 0.0)
    panel = jnp.concatenate([panel] * per_col, axis=1)
    rest_out = jnp.where(row > 0, block - update, 0.0)
    return jnp.where(first_col, panel, rest_out), log[0, 0]


def solution(mesh):
    return jax.shard_map(
        per_device,
        mesh=mesh,
        in_specs=(P("row", "col"),),
        out_specs=(P("row", "col"), P()),
        check_vma=False,
    )
```

```python
import jax
import jax.numpy as jnp
from jax import lax
from jax.experimental import pallas as pl
from jax.experimental.pallas import tpu as pltpu
from jax.sharding import PartitionSpec as P

LANES = 128
SUB = 8
TILES = LANES // SUB
GROUP = 4


def block_index(k, j, count):
    return k * count - (k * (k - 1)) // 2 + (j - k)


def leaf(a_ref, w_ref, base):
    a = [a_ref[base + t] for t in range(TILES)]
    sub = lax.broadcasted_iota(jnp.int32, (SUB, LANES), 0)
    lane = lax.broadcasted_iota(jnp.int32, (SUB, LANES), 1)
    w = [jnp.where(lane == sub + SUB * t, 1.0, 0.0).astype(jnp.float32) for t in range(TILES)]
    logs = jnp.zeros((SUB, LANES), jnp.float32)
    shape = (SUB, LANES)
    for g in range(LANES // GROUP):
        i, q, first = (GROUP * g) // SUB, (GROUP * g) % SUB, GROUP * g
        rows = [jnp.broadcast_to(a[i][q + k : q + k + 1, :], shape) for k in range(GROUP)]
        wrows = [jnp.broadcast_to(w[i][q + k : q + k + 1, :], shape) for k in range(GROUP)]
        piv = {
            (k, l): jnp.broadcast_to(rows[k][:, first + l : first + l + 1], shape)
            for k in range(GROUP)
            for l in range(k, GROUP)
        }
        scale, inv, mult = [], [], {}
        for k in range(GROUP):
            s = lax.rsqrt(piv[k, k])
            logs = logs + jnp.log(piv[k, k])
            scale.append(s)
            inv.append(s * s)
            for l in range(k + 1, GROUP):
                mult[l, k] = piv[k, l] * inv[k]
            for l in range(k + 1, GROUP):
                for m in range(l, GROUP):
                    piv[l, m] = piv[l, m] - mult[l, k] * piv[k, m]
            for l in range(k + 1, GROUP):
                rows[l] = rows[l] - mult[l, k] * rows[k]
                wrows[l] = wrows[l] - mult[l, k] * wrows[k]
        for k in range(GROUP):
            w_ref[base + i, q + k : q + k + 1, :] = (wrows[k] * scale[k])[0:1, :]
        start = i if q + GROUP < SUB else i + 1
        if start >= TILES:
            continue
        ya = [rows[k] * inv[k] for k in range(GROUP)]
        yw = [wrows[k] * inv[k] for k in range(GROUP)]
        for k in range(GROUP - 1, 0, -1):
            for l in range(k):
                ya[l] = ya[l] - mult[k, l] * ya[k]
                yw[l] = yw[l] - mult[k, l] * yw[k]
        for t in range(start, TILES):
            cols = [jnp.broadcast_to(a[t][:, first + k : first + k + 1], shape) for k in range(GROUP)]
            da = (cols[0] * ya[0] + cols[1] * ya[1]) + (cols[2] * ya[2] + cols[3] * ya[3])
            dw = (cols[0] * yw[0] + cols[1] * yw[1]) + (cols[2] * yw[2] + cols[3] * yw[3])
            a[t] = a[t] - da
            w[t] = w[t] - dw
    return logs


def mm(x, y, dims):
    return lax.dot_general(
        x, y, (dims, ((), ())), precision=lax.Precision.HIGHEST, preferred_element_type=jnp.float32
    )


def get(ref, b):
    return ref[b * TILES : (b + 1) * TILES].reshape(LANES, LANES)


def put(ref, b, value):
    ref[b * TILES : (b + 1) * TILES] = value.reshape(TILES, SUB, LANES)


def row_panel(kk, count, a, w):
    inv = get(w, block_index(kk, kk, count))
    right, left = list(range(kk + 1, count)), list(range(kk))
    src = [get(a, block_index(kk, j, count)) for j in right]
    src += [get(w, block_index(j, kk, count)) for j in left]
    if not src:
        return
    out = mm(inv, jnp.concatenate(src, axis=1), ((1,), (0,)))
    for n, j in enumerate(right):
        put(a, block_index(kk, j, count), out[:, n * LANES : (n + 1) * LANES])
    for n, j in enumerate(left, len(right)):
        put(w, block_index(j, kk, count), out[:, n * LANES : (n + 1) * LANES])


def trail(kk, count, a, w):
    for i in range(kk + 1, count):
        cols = [get(a, block_index(kk, j, count)) for j in range(i, count)]
        cols += [get(w, block_index(j, kk, count)) for j in range(kk + 1)]
        upd = mm(get(a, block_index(kk, i, count)), jnp.concatenate(cols, axis=1), ((0,), (0,)))
        n = 0
        for j in range(i, count):
            b = block_index(i, j, count)
            put(a, b, get(a, b) - upd[:, n * LANES : (n + 1) * LANES])
            n += 1
        for j in range(kk + 1):
            b = block_index(j, i, count)
            old = get(w, b) if j < kk else jnp.zeros((LANES, LANES), jnp.float32)
            put(w, b, old - upd[:, n * LANES : (n + 1) * LANES])
            n += 1


def first_panel(top, count):
    def body(top_ref, out, inv, log, a, w):
        for j in range(count):
            put(a, j, top_ref[:, j * LANES : (j + 1) * LANES])
        log[...] = leaf(a, w, 0)
        row_panel(0, count, a, w)
        for j in range(1, count):
            out[:, j * LANES : (j + 1) * LANES] = get(a, j)
        out[:, :LANES] = jnp.zeros((LANES, LANES), jnp.float32)
        inv[...] = get(w, 0)

    f32 = jnp.float32
    return pl.pallas_call(
        body,
        out_shape=[
            jax.ShapeDtypeStruct((LANES, count * LANES), f32),
            jax.ShapeDtypeStruct((LANES, LANES), f32),
            jax.ShapeDtypeStruct((SUB, LANES), f32),
        ],
        scratch_shapes=[
            pltpu.VMEM((count * TILES, SUB, LANES), f32),
            pltpu.VMEM((TILES, SUB, LANES), f32),
        ],
        name="first_panel",
    )(top)


def other_panels(top, inv, log, rest, count):
    blocks = count * (count + 1) // 2

    def body(top_ref, inv_ref, log_ref, rest_ref, inverse, log, a, w):
        for j in range(1, count):
            put(a, j, top_ref[:, j * LANES : (j + 1) * LANES])
        for b in range(count, blocks):
            n = b - count
            put(a, b, rest_ref[:, n * LANES : (n + 1) * LANES])
        put(w, 0, inv_ref[...])
        log[...] = log_ref[...]
        trail(0, count, a, w)

        def step(k, carry):
            base = TILES * (k * count - (k * (k - 1)) // 2)
            log[...] = log[...] + leaf(a, w, base)
            for kk in range(1, count):

                @pl.when(k == kk)
                def _():
                    row_panel(kk, count, a, w)
                    trail(kk, count, a, w)

            return carry

        lax.fori_loop(1, count, step, 0)
        for i in range(count):
            for j in range(count):
                value = get(w, block_index(j, i, count)) if j <= i else jnp.zeros((LANES, LANES), jnp.float32)
                inverse[i * LANES : (i + 1) * LANES, j * LANES : (j + 1) * LANES] = value

    f32 = jnp.float32
    return pl.pallas_call(
        body,
        out_shape=[
            jax.ShapeDtypeStruct((count * LANES, count * LANES), f32),
            jax.ShapeDtypeStruct((SUB, LANES), f32),
        ],
        scratch_shapes=[
            pltpu.VMEM((blocks * TILES, SUB, LANES), f32),
            pltpu.VMEM((blocks * TILES, SUB, LANES), f32),
        ],
        name="other_panels",
    )(top, inv, log, rest)


def tree_rounds(value, axes, strides, have=(0,)):
    index = lax.axis_index(axes)
    have = list(have)
    for stride in strides:
        got = lax.ppermute(value, axes, [(s, s + stride) for s in have])
        value = jnp.where((index // stride) % 2 == 1, got, value)
        have = have + [s + stride for s in have]
    return value


def reach(strides):
    have = [0]
    for stride in strides:
        have = have + [s + stride for s in have]
    return have


def halvings(size, unit=1):
    out = []
    while size > 1:
        size //= 2
        out.append(size * unit)
    return out


def per_device(block):
    width, cols = block.shape
    both = ("row", "col")
    rows_n, cols_n = lax.axis_size("row"), lax.axis_size("col")
    row = lax.axis_index("row")
    col = lax.axis_index("col")
    count = width // LANES
    per_col = cols // width

    first = block[:LANES, :width]
    rest = jnp.concatenate(
        [block[k * LANES : (k + 1) * LANES, k * LANES : width] for k in range(1, count)], axis=1
    )
    row_strides, col_strides = halvings(rows_n, cols_n), halvings(cols_n)
    order = row_strides[-1:] + row_strides[:-1] + col_strides
    first = tree_rounds(first, both, row_strides)
    rest = tree_rounds(rest, both, order[:1])
    own = tree_rounds(block[:, :width], "col", col_strides[:-1])
    first, rest, own = lax.optimization_barrier((first, rest, own))
    own = tree_rounds(own, "col", col_strides[-1:], range(0, cols_n, 2))
    first = tree_rounds(first, both, col_strides, range(0, rows_n * cols_n, cols_n))
    rest = tree_rounds(rest, both, order[1:-2], reach(order[:1]))

    far = own
    low, size = 0, 1
    while size < cols_n:
        moves = [
            (low + i, low - 1 - i if i < size // 2 else low + 2 * size - 1 - i) for i in range(size)
        ]
        if 2 * size == cols_n:
            first, rest, far = lax.optimization_barrier((first, rest, far))
        got = lax.ppermute(
            far,
            both,
            [
                (
                    (((c + src) % cols_n) * per_col + b) * cols_n + c,
                    (((c + dst) % cols_n) * per_col + b) * cols_n + c,
                )
                for c in range(cols_n)
                for b in range(per_col)
                for src, dst in moves
            ],
        )
        offset = (row // per_col - col) % cols_n
        takes = jnp.zeros((), bool)
        for _, dst in moves:
            takes = takes | (offset == dst % cols_n)
        far = jnp.where(takes, got, far)
        low, size = low - size // 2, 2 * size

    rest = tree_rounds(rest, both, order[-2:-1], reach(order[:-2]))
    top, inv, log = first_panel(first, count)
    top, rest, far = lax.optimization_barrier((top, rest, far))
    rest = tree_rounds(rest, both, order[-1:], reach(order[:-1]))
    parts = jnp.zeros((per_col, width, width), jnp.float32)
    parts = lax.dynamic_update_slice(parts, far[None], (row % per_col, 0, 0))
    for s in range(1, per_col):
        pairs = [(r, r - r % per_col + (r % per_col + s) % per_col) for r in range(rows_n)]
        got = lax.ppermute(far, "row", pairs)
        parts = lax.dynamic_update_slice(parts, got[None], ((row - s) % per_col, 0, 0))
    far = parts.reshape(cols, width)
    inverse, log = other_panels(top, inv, log, rest, count)

    high = lax.Precision.HIGH
    across = (((1,), (1,)), ((), ()))
    panel = lax.dot_general(own, inverse, across, precision=high)
    other = lax.dot_general(far, inverse, across, precision=high)
    update = lax.dot_general(panel, other, across, precision=high)
    col_block = per_col * col + jnp.arange(cols, dtype=jnp.int32) // width
    first_col = (col_block == 0)[None, :]
    in_row = jnp.arange(width, dtype=jnp.int32)
    keep = (row > 0) | (in_row[:, None] >= in_row[None, :])
    panel = jnp.where(keep, panel, 0.0)
    panel = jnp.concatenate([panel] * per_col, axis=1)
    rest_out = jnp.where(row > 0, block - update, 0.0)
    return jnp.where(first_col, panel, rest_out), log[0, 0]


def solution(mesh):
    return jax.shard_map(
        per_device,
        mesh=mesh,
        in_specs=(P("row", "col"),),
        out_specs=(P("row", "col"), P()),
        check_vma=False,
    )
```

```python
import jax
import jax.numpy as jnp
from jax import lax
from jax.experimental import pallas as pl
from jax.experimental.pallas import tpu as pltpu
from jax.sharding import PartitionSpec as P

LANES = 128
SUB = 8
TILES = LANES // SUB
GROUP = 4


def block_index(k, j, count):
    return k * count - (k * (k - 1)) // 2 + (j - k)


def leaf(a_ref, w_ref, base):
    a = [a_ref[base + t] for t in range(TILES)]
    sub = lax.broadcasted_iota(jnp.int32, (SUB, LANES), 0)
    lane = lax.broadcasted_iota(jnp.int32, (SUB, LANES), 1)
    w = [jnp.where(lane == sub + SUB * t, 1.0, 0.0).astype(jnp.float32) for t in range(TILES)]
    logs = jnp.zeros((SUB, LANES), jnp.float32)
    shape = (SUB, LANES)
    for g in range(LANES // GROUP):
        i, q, first = (GROUP * g) // SUB, (GROUP * g) % SUB, GROUP * g
        rows = [jnp.broadcast_to(a[i][q + k : q + k + 1, :], shape) for k in range(GROUP)]
        wrows = [jnp.broadcast_to(w[i][q + k : q + k + 1, :], shape) for k in range(GROUP)]
        piv = {
            (k, l): jnp.broadcast_to(rows[k][:, first + l : first + l + 1], shape)
            for k in range(GROUP)
            for l in range(k, GROUP)
        }
        scale, inv, mult = [], [], {}
        for k in range(GROUP):
            s = lax.rsqrt(piv[k, k])
            logs = logs + jnp.log(piv[k, k])
            scale.append(s)
            inv.append(s * s)
            for l in range(k + 1, GROUP):
                mult[l, k] = piv[k, l] * inv[k]
            for l in range(k + 1, GROUP):
                for m in range(l, GROUP):
                    piv[l, m] = piv[l, m] - mult[l, k] * piv[k, m]
            for l in range(k + 1, GROUP):
                rows[l] = rows[l] - mult[l, k] * rows[k]
                wrows[l] = wrows[l] - mult[l, k] * wrows[k]
        for k in range(GROUP):
            w_ref[base + i, q + k : q + k + 1, :] = (wrows[k] * scale[k])[0:1, :]
        start = i if q + GROUP < SUB else i + 1
        if start >= TILES:
            continue
        ya = [rows[k] * inv[k] for k in range(GROUP)]
        yw = [wrows[k] * inv[k] for k in range(GROUP)]
        for k in range(GROUP - 1, 0, -1):
            for l in range(k):
                ya[l] = ya[l] - mult[k, l] * ya[k]
                yw[l] = yw[l] - mult[k, l] * yw[k]
        for t in range(start, TILES):
            cols = [jnp.broadcast_to(a[t][:, first + k : first + k + 1], shape) for k in range(GROUP)]
            da = (cols[0] * ya[0] + cols[1] * ya[1]) + (cols[2] * ya[2] + cols[3] * ya[3])
            dw = (cols[0] * yw[0] + cols[1] * yw[1]) + (cols[2] * yw[2] + cols[3] * yw[3])
            a[t] = a[t] - da
            w[t] = w[t] - dw
    return logs


def mm(x, y, dims):
    return lax.dot_general(
        x, y, (dims, ((), ())), precision=lax.Precision.HIGHEST, preferred_element_type=jnp.float32
    )


def get(ref, b):
    return ref[b * TILES : (b + 1) * TILES].reshape(LANES, LANES)


def put(ref, b, value):
    ref[b * TILES : (b + 1) * TILES] = value.reshape(TILES, SUB, LANES)


def row_panel(kk, count, a, w):
    inv = get(w, block_index(kk, kk, count))
    right, left = list(range(kk + 1, count)), list(range(kk))
    src = [get(a, block_index(kk, j, count)) for j in right]
    src += [get(w, block_index(j, kk, count)) for j in left]
    if not src:
        return
    out = mm(inv, jnp.concatenate(src, axis=1), ((1,), (0,)))
    for n, j in enumerate(right):
        put(a, block_index(kk, j, count), out[:, n * LANES : (n + 1) * LANES])
    for n, j in enumerate(left, len(right)):
        put(w, block_index(j, kk, count), out[:, n * LANES : (n + 1) * LANES])


def trail(kk, count, a, w):
    for i in range(kk + 1, count):
        cols = [get(a, block_index(kk, j, count)) for j in range(i, count)]
        cols += [get(w, block_index(j, kk, count)) for j in range(kk + 1)]
        upd = mm(get(a, block_index(kk, i, count)), jnp.concatenate(cols, axis=1), ((0,), (0,)))
        n = 0
        for j in range(i, count):
            b = block_index(i, j, count)
            put(a, b, get(a, b) - upd[:, n * LANES : (n + 1) * LANES])
            n += 1
        for j in range(kk + 1):
            b = block_index(j, i, count)
            old = get(w, b) if j < kk else jnp.zeros((LANES, LANES), jnp.float32)
            put(w, b, old - upd[:, n * LANES : (n + 1) * LANES])
            n += 1


def first_panel(top, count):
    def body(top_ref, out, inv, log, a, w):
        for j in range(count):
            put(a, j, top_ref[:, j * LANES : (j + 1) * LANES])
        log[...] = leaf(a, w, 0)
        row_panel(0, count, a, w)
        for j in range(1, count):
            out[:, j * LANES : (j + 1) * LANES] = get(a, j)
        out[:, :LANES] = jnp.zeros((LANES, LANES), jnp.float32)
        inv[...] = get(w, 0)

    f32 = jnp.float32
    return pl.pallas_call(
        body,
        out_shape=[
            jax.ShapeDtypeStruct((LANES, count * LANES), f32),
            jax.ShapeDtypeStruct((LANES, LANES), f32),
            jax.ShapeDtypeStruct((SUB, LANES), f32),
        ],
        scratch_shapes=[
            pltpu.VMEM((count * TILES, SUB, LANES), f32),
            pltpu.VMEM((TILES, SUB, LANES), f32),
        ],
        name="first_panel",
    )(top)


def other_panels(top, inv, log, rest, count):
    blocks = count * (count + 1) // 2

    def body(top_ref, inv_ref, log_ref, rest_ref, inverse, log, a, w):
        for j in range(1, count):
            put(a, j, top_ref[:, j * LANES : (j + 1) * LANES])
        for b in range(count, blocks):
            n = b - count
            put(a, b, rest_ref[:, n * LANES : (n + 1) * LANES])
        put(w, 0, inv_ref[...])
        log[...] = log_ref[...]
        trail(0, count, a, w)

        def step(k, carry):
            base = TILES * (k * count - (k * (k - 1)) // 2)
            log[...] = log[...] + leaf(a, w, base)
            for kk in range(1, count):

                @pl.when(k == kk)
                def _():
                    row_panel(kk, count, a, w)
                    trail(kk, count, a, w)

            return carry

        lax.fori_loop(1, count, step, 0)
        for i in range(count):
            for j in range(count):
                value = get(w, block_index(j, i, count)) if j <= i else jnp.zeros((LANES, LANES), jnp.float32)
                inverse[i * LANES : (i + 1) * LANES, j * LANES : (j + 1) * LANES] = value

    f32 = jnp.float32
    return pl.pallas_call(
        body,
        out_shape=[
            jax.ShapeDtypeStruct((count * LANES, count * LANES), f32),
            jax.ShapeDtypeStruct((SUB, LANES), f32),
        ],
        scratch_shapes=[
            pltpu.VMEM((blocks * TILES, SUB, LANES), f32),
            pltpu.VMEM((blocks * TILES, SUB, LANES), f32),
        ],
        name="other_panels",
    )(top, inv, log, rest)


def tree_rounds(value, axes, strides, have=(0,)):
    index = lax.axis_index(axes)
    have = list(have)
    for stride in strides:
        got = lax.ppermute(value, axes, [(s, s + stride) for s in have])
        value = jnp.where((index // stride) % 2 == 1, got, value)
        have = have + [s + stride for s in have]
    return value


def reach(strides):
    have = [0]
    for stride in strides:
        have = have + [s + stride for s in have]
    return have


def halvings(size, unit=1):
    out = []
    while size > 1:
        size //= 2
        out.append(size * unit)
    return out


def per_device(block):
    width, cols = block.shape
    both = ("row", "col")
    rows_n, cols_n = lax.axis_size("row"), lax.axis_size("col")
    row = lax.axis_index("row")
    col = lax.axis_index("col")
    count = width // LANES
    per_col = cols // width

    first = block[:LANES, :width]
    rest = jnp.concatenate(
        [block[k * LANES : (k + 1) * LANES, k * LANES : width] for k in range(1, count)], axis=1
    )
    row_strides, col_strides = halvings(rows_n, cols_n), halvings(cols_n)
    order = row_strides[-1:] + row_strides[:-1] + col_strides
    first = tree_rounds(first, both, row_strides)
    rest = tree_rounds(rest, both, order[:1])
    own = tree_rounds(block[:, :width], "col", col_strides[:-1])
    first, rest, own = lax.optimization_barrier((first, rest, own))
    own = tree_rounds(own, "col", col_strides[-1:], range(0, cols_n, 2))
    first = tree_rounds(first, both, col_strides, range(0, rows_n * cols_n, cols_n))
    rest = tree_rounds(rest, both, order[1:-2], reach(order[:1]))

    far = own
    low, size = 0, 1
    while size < cols_n:
        moves = [
            (low + i, low - 1 - i if i < size // 2 else low + 2 * size - 1 - i) for i in range(size)
        ]
        if 2 * size == cols_n:
            first, rest, far = lax.optimization_barrier((first, rest, far))
        got = lax.ppermute(
            far,
            both,
            [
                (
                    (((c + src) % cols_n) * per_col + b) * cols_n + c,
                    (((c + dst) % cols_n) * per_col + b) * cols_n + c,
                )
                for c in range(cols_n)
                for b in range(per_col)
                for src, dst in moves
            ],
        )
        offset = (row // per_col - col) % cols_n
        takes = jnp.zeros((), bool)
        for _, dst in moves:
            takes = takes | (offset == dst % cols_n)
        far = jnp.where(takes, got, far)
        low, size = low - size // 2, 2 * size

    rest = tree_rounds(rest, both, order[-2:-1], reach(order[:-2]))
    top, inv, log = first_panel(first, count)
    top, rest = lax.optimization_barrier((top, rest))
    rest = tree_rounds(rest, both, order[-1:], reach(order[:-1]))
    top, far = lax.optimization_barrier((top, far))
    parts = jnp.zeros((per_col, width, width), jnp.float32)
    parts = lax.dynamic_update_slice(parts, far[None], (row % per_col, 0, 0))
    for s in range(1, per_col):
        pairs = [(r, r - r % per_col + (r % per_col + s) % per_col) for r in range(rows_n)]
        got = lax.ppermute(far, "row", pairs)
        parts = lax.dynamic_update_slice(parts, got[None], ((row - s) % per_col, 0, 0))
    far = parts.reshape(cols, width)
    inverse, log = other_panels(top, inv, log, rest, count)

    high = lax.Precision.HIGH
    across = (((1,), (1,)), ((), ()))
    panel = lax.dot_general(own, inverse, across, precision=high)
    other = lax.dot_general(far, inverse, across, precision=high)
    update = lax.dot_general(panel, other, across, precision=high)
    col_block = per_col * col + jnp.arange(cols, dtype=jnp.int32) // width
    first_col = (col_block == 0)[None, :]
    in_row = jnp.arange(width, dtype=jnp.int32)
    keep = (row > 0) | (in_row[:, None] >= in_row[None, :])
    panel = jnp.where(keep, panel, 0.0)
    panel = jnp.concatenate([panel] * per_col, axis=1)
    rest_out = jnp.where(row > 0, block - update, 0.0)
    return jnp.where(first_col, panel, rest_out), log[0, 0]


def solution(mesh):
    return jax.shard_map(
        per_device,
        mesh=mesh,
        in_specs=(P("row", "col"),),
        out_specs=(P("row", "col"), P()),
        check_vma=False,
    )
```
